64 devices in a mesh: dp: 8 (over x, y, core), tp: 8 (over z).
Axes of the slice: x: 2, y: 2, z: 8, core: 2. Of those that a mesh axis runs over, the one named last changes fastest.
The devices are a block of a 4x4x8 slice.
Arguments:
- x: bfloat16 [16384, 4096], P(('dp', 'tp')), parts along dimension 0
- w_gate: bfloat16 [4096, 16384], P(None, 'tp')
- w_up: bfloat16 [4096, 16384], P(None, 'tp')
- w_down: bfloat16 [16384, 4096], P('tp')
Outputs:
- output: bfloat16 [16384, 4096], P(('dp', 'tp')), parts along dimension 0
There are 8 independent parts. The reference program is written for one: setup_inputs(seed, part) draws one part's arguments, and reference() takes and returns one part's arrays. A program takes and returns all parts, laid end to end along the dimension named above; an argument that names none is the same for every part.
All inputs are finite; a program needn't handle non-finite values.
Results may differ from the reference program's by a relative error of at most 0.016.
Values are sent between devices in bfloat16 or wider.
A program may use at most 768 MiB of HBM per device.

```python
import jax
import jax.numpy as jnp

ROWS = 2048
D = 4096
FF = 16384


def setup_inputs(seed: int = 0, part: int = 0) -> dict:
    kx, kg, ku, kd = jax.random.split(jax.random.key(seed), 4)
    drawn = {
        "x": jax.random.normal(jax.random.fold_in(kx, part), (ROWS, D), jnp.float32),
        "w_gate": jax.random.normal(kg, (D, FF), jnp.float32) * D**-0.5,
        "w_up": jax.random.normal(ku, (D, FF), jnp.float32) * D**-0.5,
        "w_down": jax.random.normal(kd, (FF, D), jnp.float32) * FF**-0.5,
    }
    return {k: v.astype(jnp.bfloat16) for k, v in drawn.items()}


def reference(x, w_gate, w_up, w_down):
    gate = jnp.dot(x, w_gate, preferred_element_type=jnp.float32)
    up = jnp.dot(x, w_up, preferred_element_type=jnp.float32)
    hidden = (jax.nn.silu(gate) * up).astype(jnp.bfloat16)
    return jnp.dot(hidden, w_down, preferred_element_type=jnp.float32).astype(jnp.bfloat16)
```

```python
import jax
import jax.numpy as jnp
from jax import lax
from jax.sharding import PartitionSpec as P

CHUNKS = 2


def solution(mesh):
    def mlp(rows, w_gate, w_up, w_down):
        gate = jnp.dot(rows, w_gate, preferred_element_type=jnp.float32)
        up = jnp.dot(rows, w_up, preferred_element_type=jnp.float32)
        hidden = (jax.nn.silu(gate) * up).astype(jnp.bfloat16)
        return jnp.dot(hidden, w_down, preferred_element_type=jnp.float32).astype(jnp.bfloat16)

    def step(x, w_gate, w_up, w_down):
        size = x.shape[0] // CHUNKS
        rows = [
            lax.all_gather(x[c * size : (c + 1) * size], "tp", axis=0, tiled=True)
            for c in range(CHUNKS)
        ]
        done = []
        for c in range(CHUNKS):
            term = mlp(rows[c], w_gate, w_up, w_down)
            done.append(lax.psum_scatter(term, "tp", scatter_dimension=0, tiled=True))
        return jnp.concatenate(done, axis=0)

    return jax.shard_map(
        step,
        mesh=mesh,
        in_specs=(P(("dp", "tp"), None), P(None, "tp"), P(None, "tp"), P("tp", None)),
        out_specs=P(("dp", "tp"), None),
        check_vma=False,
    )
```

```python
import functools

import jax
import jax.numpy as jnp
from jax import lax
from jax.experimental import pallas as pl
from jax.experimental.pallas import tpu as pltpu
from jax.sharding import PartitionSpec as P

MESH = pl.DeviceIdType.MESH
F32 = jnp.float32
BF16 = jnp.bfloat16
FT = 256
SLOTS = 3
NT = 512


def kernel(
    n, x_ref, wg_ref, wu_ref, wd_ref, y_ref,
    buf, hid, wd, wt, own, ag_send, ag_recv, rs_send, rs_recv, w_sem, wd_sem, x_sem, y_sem,
):
    me = lax.axis_index("tp")
    right, left = lax.rem(me + 1, n), lax.rem(me + n - 1, n)
    steps = n - 1
    rc = x_ref.shape[0] // 2
    pc = rc // 2
    d_model = x_ref.shape[1]
    ff = wg_ref.shape[1]
    tiles = ff // FT
    per = tiles // 2
    n_tiles = 2 * n * per

    def rows(block, part=0, size=pc):
        return pl.ds(pl.multiple_of(block * rc + part * pc, pc), size)

    def own_block(c):
        return 2 * n - 1 - n * c

    def ag_copy(d, c, i, src):
        return pltpu.make_async_remote_copy(
            src_ref=buf.at[src],
            dst_ref=buf.at[rows(c * n + i, d)],
            send_sem=ag_send.at[d, c * steps + i],
            recv_sem=ag_recv.at[d, c * steps + i],
            device_id={"tp": (right, left)[d]},
            device_id_type=MESH,
        )

    def arrived_sum(c, r):
        return 2 * n * (1 - c) + r

    def rs_copy(d, c, r, block):
        return pltpu.make_async_remote_copy(
            src_ref=buf.at[rows(block, d)],
            dst_ref=buf.at[rows(arrived_sum(c, r), d)],
            send_sem=rs_send.at[d, c * steps + r],
            recv_sem=rs_recv.at[d, c * steps + r],
            device_id={"tp": (left, right)[d]},
            device_id_type=MESH,
        )

    def w_copies(g):
        slot = g % SLOTS
        col = pl.ds(pl.multiple_of((g % tiles) * FT, FT), FT)
        return [
            pltpu.make_async_copy(ref.at[:, col], wt.at[slot, :, pl.ds(k * FT, FT)], w_sem.at[k, slot])
            for k, ref in enumerate((wg_ref, wu_ref))
        ]

    x_copies = [
        pltpu.make_async_copy(
            x_ref.at[pl.ds(c * rc, rc)], buf.at[rows(own_block(c), 0, rc)], x_sem.at[c]
        )
        for c in range(2)
    ]
    for copy in x_copies:
        copy.start()

    barrier = pltpu.get_barrier_semaphore()
    for neighbour in (left, right):
        pl.semaphore_signal(barrier, inc=1, device_id={"tp": neighbour}, device_id_type=MESH)
    pl.semaphore_wait(barrier, 2)

    def send_own(c):
        for i in range(2):
            for d in range(2):
                ag_copy(d, c, i, rows(own_block(c), i ^ d)).start()

    x_copies[0].wait()
    send_own(0)
    x_copies[1].wait()
    for g in range(SLOTS - 1):
        for copy in w_copies(g):
            copy.start()
    wd_copy = pltpu.make_async_copy(wd_ref, wd, wd_sem)
    wd_copy.start()

    def hidden_half(q):
        lhs = pl.ds(pl.multiple_of((q // 2) * 2 * rc, 2 * rc), 2 * rc)

        @pl.loop(0, per)
        def _(j):
            g = q * per + j
            slot = g % SLOTS
            for copy in w_copies(g):
                copy.wait()

            @pl.when(g + SLOTS - 1 < n_tiles)
            def _():
                for copy in w_copies(g + SLOTS - 1):
                    copy.start()

            both = jnp.dot(buf[lhs, :], wt[slot], preferred_element_type=F32)
            gate, up = both[:, :FT], both[:, FT:]
            col = pl.ds(pl.multiple_of((g % tiles) * FT, FT), FT)
            hid[lhs, col] = (jax.nn.silu(gate) * up).astype(BF16)

    def down(block, col):
        return jnp.dot(hid[rows(block, 0, rc), :], wd[:, col], preferred_element_type=F32)

    def down_tiles(body):
        @pl.loop(0, d_model // NT)
        def _(j):
            body(pl.ds(pl.multiple_of(j * NT, NT), NT))

    def send_sum(c, r, add):
        block = arrived_sum(c, r - 2) if add else c * n + n - 2 + r
        dst = rows(block, 0, rc)

        def body(col):
            term = down(c * n + n - 2 - r, col)
            if add:
                term = term + buf[dst, col].astype(F32)
            buf[dst, col] = term.astype(BF16)

        down_tiles(body)
        for d in range(2):
            rs_copy(d, c, r, block).start()

    def wait_sum(c, r):
        for d in range(2):
            rs_copy(d, c, r, arrived_sum(c, r)).wait_recv()

    def swapped(block, col):
        return jnp.concatenate([buf[rows(block, 1), col], buf[rows(block, 0), col]], axis=0).astype(F32)

    def y_copy(c):
        return pltpu.make_async_copy(
            buf.at[rows(arrived_sum(c, steps - 1), 0, rc)], y_ref.at[pl.ds(c * rc, rc)], y_sem.at[c]
        )

    @pl.loop(0, 4 * steps - 2)
    def _(t):
        @pl.when(t < 2 * steps)
        def _():
            c, i = t // steps, t % steps
            for d in range(2):
                ag_copy(d, c, i, rows(c * n + i, d)).wait_recv()

            @pl.when(i < steps - 2)
            def _():
                for d in range(2):
                    ag_copy(d, c, i + 2, rows(c * n + i, d)).start()

        @pl.when(t == steps - 2)
        def _():
            send_own(1)

        @pl.when((t >= 1) & (t <= 2 * steps))
        def _():
            a = t - 1
            for d in range(2):
                ag_copy(d, a // steps, a % steps, rows((a // steps) * n + a % steps, d)).wait_send()

        @pl.when(t >= 2 * steps + 1)
        def _():
            u = t - (2 * steps + 1)
            for d in range(2):
                rs_copy(d, u // steps, u % steps, arrived_sum(u // steps, u % steps)).wait_send()

        @pl.when(t == 2 * steps - 2)
        def _():
            wd_copy.wait()

        @pl.when(t >= 2 * steps - 2)
        def _():
            u = t - (2 * steps - 2)
            c, r = u // steps, u % steps

            @pl.when(r < 2)
            def _():
                send_sum(c, r, False)

            @pl.when(r >= 2)
            def _():
                wait_sum(c, r - 2)
                send_sum(c, r, True)

        @pl.when((t >= 1) & (t <= 2 * n))
        def _():
            hidden_half(t - 1)

        @pl.when(t == 3 * steps - 1)
        def _():
            wait_sum(0, steps - 2)
            wait_sum(0, steps - 1)
            last = arrived_sum(0, steps - 1)
            dst = rows(last, 0, rc)

            def body(col):
                total = down(own_block(0), col) + swapped(last - 1, col) + buf[dst, col].astype(F32)
                buf[dst, col] = total.astype(BF16)

            down_tiles(body)
            y_copy(0).start()

    wait_sum(1, steps - 2)
    last = arrived_sum(1, steps - 1)
    dst = rows(last, 0, rc)

    def partial(col):
        own[:, col] = down(own_block(1), col) + swapped(last - 1, col)

    down_tiles(partial)
    wait_sum(1, steps - 1)

    def finish(col):
        buf[dst, col] = (own[:, col] + buf[dst, col].astype(F32)).astype(BF16)

    down_tiles(finish)
    y_copy(1).start()
    for u in range(2 * steps - 3, 2 * steps):
        for d in range(2):
            rs_copy(d, u // steps, u % steps, arrived_sum(u // steps, u % steps)).wait_send()
    for c in range(2):
        y_copy(c).wait()


def solution(mesh):
    n = mesh.shape["tp"]

    def step(x, w_gate, w_up, w_down):
        (m, d_model), ff = x.shape, w_gate.shape[1]
        rc = m // 2
        steps = n - 1
        hbm = pl.BlockSpec(memory_space=pltpu.HBM)
        return pl.pallas_call(
            functools.partial(kernel, n),
            out_shape=jax.ShapeDtypeStruct(x.shape, BF16),
            in_specs=[hbm] * 4,
            out_specs=hbm,
            scratch_shapes=[
                pltpu.VMEM(((3 * n - 1) * rc, d_model), BF16),
                pltpu.VMEM((2 * n * rc, ff), BF16),
                pltpu.VMEM((ff, d_model), BF16),
                pltpu.VMEM((SLOTS, d_model, 2 * FT), BF16),
                pltpu.VMEM((rc, d_model), F32),
                pltpu.SemaphoreType.DMA((2, 2 * steps)),
                pltpu.SemaphoreType.DMA((2, 2 * steps)),
                pltpu.SemaphoreType.DMA((2, 2 * steps)),
                pltpu.SemaphoreType.DMA((2, 2 * steps)),
                pltpu.SemaphoreType.DMA((2, SLOTS)),
                pltpu.SemaphoreType.DMA,
                pltpu.SemaphoreType.DMA((2,)),
                pltpu.SemaphoreType.DMA((2,)),
            ],
            compiler_params=pltpu.CompilerParams(
                collective_id=0, has_side_effects=True, vmem_limit_bytes=67043328
            ),
            name="mlp_ring",
        )(x, w_gate, w_up, w_down)

    return jax.shard_map(
        step,
        mesh=mesh,
        in_specs=(P(("dp", "tp"), None), P(None, "tp"), P(None, "tp"), P("tp", None)),
        out_specs=P(("dp", "tp"), None),
        check_vma=False,
    )
```

```python
import functools

import jax
import jax.numpy as jnp
from jax import lax
from jax.experimental import pallas as pl
from jax.experimental.pallas import tpu as pltpu
from jax.sharding import PartitionSpec as P

MESH = pl.DeviceIdType.MESH
F32 = jnp.float32
BF16 = jnp.bfloat16
FT = 256
SLOTS = 3
NT = 512
VMEM_LIMIT = 51 * 1024 * 1024


def kernel(
    n, x_ref, wg_ref, wu_ref, wd_ref, y_ref,
    buf, hid, wd, wt, own, ag_send, ag_recv, rs_send, rs_recv, w_sem, wd_sem, x_sem,
):
    me = lax.axis_index("tp")
    right, left = lax.rem(me + 1, n), lax.rem(me + n - 1, n)
    steps = n - 1
    rc = x_ref.shape[0] // 2
    pc = rc // 2
    d_model = x_ref.shape[1]
    ff = wg_ref.shape[1]
    tiles = ff // FT
    per = tiles // 2
    halves = 2 * n * per * 2
    kd = d_model // 2

    def rows(block, part=0, size=pc):
        return pl.ds(pl.multiple_of(block * rc + part * pc, pc), size)

    def own_block(c):
        return 2 * n - 1 - n * c

    def ag_copy(d, c, i, src):
        return pltpu.make_async_remote_copy(
            src_ref=buf.at[src],
            dst_ref=buf.at[rows(c * n + i, d)],
            send_sem=ag_send.at[d, c * steps + i],
            recv_sem=ag_recv.at[d, c * steps + i],
            device_id={"tp": (right, left)[d]},
            device_id_type=MESH,
        )

    def arrived_sum(c, r):
        return c * n + r

    def rs_copy(d, c, r, block):
        return pltpu.make_async_remote_copy(
            src_ref=buf.at[rows(block, d)],
            dst_ref=buf.at[rows(arrived_sum(c, r), d)],
            send_sem=rs_send.at[d, c * steps + r],
            recv_sem=rs_recv.at[d, c * steps + r],
            device_id={"tp": (left, right)[d]},
            device_id_type=MESH,
        )

    def w_copies(g):
        slot = g % SLOTS
        row = pl.ds(pl.multiple_of((g % 2) * kd, kd), kd)
        col = pl.ds(pl.multiple_of((g // 2 % tiles) * FT, FT), FT)
        return [
            pltpu.make_async_copy(ref.at[row, col], wt.at[slot, :, pl.ds(k * FT, FT)], w_sem.at[k, slot])
            for k, ref in enumerate((wg_ref, wu_ref))
        ]

    x_copies = [
        pltpu.make_async_copy(
            x_ref.at[pl.ds(c * rc, rc)], buf.at[rows(own_block(c), 0, rc)], x_sem.at[c]
        )
        for c in range(2)
    ]
    for copy in x_copies:
        copy.start()

    barrier = pltpu.get_barrier_semaphore()
    for neighbour in (left, right):
        pl.semaphore_signal(barrier, inc=1, device_id={"tp": neighbour}, device_id_type=MESH)
    pl.semaphore_wait(barrier, 2)

    def send_own(c):
        for i in range(2):
            for d in range(2):
                ag_copy(d, c, i, rows(own_block(c), i ^ d)).start()

    x_copies[0].wait()
    send_own(0)
    x_copies[1].wait()
    for g in range(SLOTS - 1):
        for copy in w_copies(g):
            copy.start()
    wd_copy = pltpu.make_async_copy(wd_ref, wd, wd_sem)
    wd_copy.start()

    def hidden_half(q):
        lhs = pl.ds(pl.multiple_of((q // 2) * 2 * rc, 2 * rc), 2 * rc)

        @pl.loop(0, per)
        def _(j):
            g = q * per + j
            both = None
            for k in range(2):
                i = 2 * g + k
                for copy in w_copies(i):
                    copy.wait()

                @pl.when(i + SLOTS - 1 < halves)
                def _():
                    for copy in w_copies(i + SLOTS - 1):
                        copy.start()

                part = jnp.dot(
                    buf[lhs, pl.ds(k * kd, kd)], wt[i % SLOTS], preferred_element_type=F32
                )
                both = part if both is None else both + part
            gate, up = both[:, :FT], both[:, FT:]
            col = pl.ds(pl.multiple_of((g % tiles) * FT, FT), FT)
            hid[lhs, col] = (jax.nn.silu(gate) * up).astype(BF16)

    def down(block, col):
        return jnp.dot(hid[rows(block, 0, rc), :], wd[:, col], preferred_element_type=F32)

    def down_tiles(body):
        @pl.loop(0, d_model // NT)
        def _(j):
            body(pl.ds(pl.multiple_of(j * NT, NT), NT))

    def send_sum(c, r, add):
        block = arrived_sum(c, r - 2) if add else c * n + n - 2 + r
        dst = rows(block, 0, rc)

        def body(col):
            term = down(c * n + n - 2 - r, col)
            if add:
                term = term + buf[dst, col].astype(F32)
            buf[dst, col] = term.astype(BF16)

        down_tiles(body)
        for d in range(2):
            rs_copy(d, c, r, block).start()

    def wait_sum(c, r):
        for d in range(2):
            rs_copy(d, c, r, arrived_sum(c, r)).wait_recv()

    def swapped(block, col):
        return jnp.concatenate([buf[rows(block, 1), col], buf[rows(block, 0), col]], axis=0).astype(F32)

    @pl.loop(0, 4 * steps - 2)
    def _(t):
        @pl.when(t < 2 * steps)
        def _():
            c, i = t // steps, t % steps
            for d in range(2):
                ag_copy(d, c, i, rows(c * n + i, d)).wait_recv()

            @pl.when(i < steps - 2)
            def _():
                for d in range(2):
                    ag_copy(d, c, i + 2, rows(c * n + i, d)).start()

        @pl.when(t == steps - 2)
        def _():
            send_own(1)

        @pl.when((t >= 1) & (t <= 2 * steps))
        def _():
            a = t - 1
            for d in range(2):
                ag_copy(d, a // steps, a % steps, rows((a // steps) * n + a % steps, d)).wait_send()

        @pl.when(t >= 2 * steps + 1)
        def _():
            u = t - (2 * steps + 1)
            for d in range(2):
                rs_copy(d, u // steps, u % steps, arrived_sum(u // steps, u % steps)).wait_send()

        @pl.when(t == 2 * steps - 2)
        def _():
            wd_copy.wait()

        @pl.when(t >= 2 * steps - 2)
        def _():
            u = t - (2 * steps - 2)
            c, r = u // steps, u % steps

            @pl.when(r < 2)
            def _():
                send_sum(c, r, False)

            @pl.when(r >= 2)
            def _():
                wait_sum(c, r - 2)
                send_sum(c, r, True)

        @pl.when((t >= 1) & (t <= 2 * n))
        def _():
            hidden_half(t - 1)

        @pl.when(t == 3 * steps - 1)
        def _():
            wait_sum(0, steps - 2)
            wait_sum(0, steps - 1)
            last = arrived_sum(0, steps - 1)
            dst = rows(last, 0, rc)

            def body(col):
                total = down(own_block(0), col) + swapped(last - 1, col) + buf[dst, col].astype(F32)
                y_ref[pl.ds(0, rc), col] = total.astype(BF16)

            down_tiles(body)

    wait_sum(1, steps - 2)
    last = arrived_sum(1, steps - 1)
    dst = rows(last, 0, rc)

    def partial(col):
        own[:, col] = down(own_block(1), col) + swapped(last - 1, col)

    down_tiles(partial)
    wait_sum(1, steps - 1)

    def finish(col):
        y_ref[pl.ds(rc, rc), col] = (own[:, col] + buf[dst, col].astype(F32)).astype(BF16)

    down_tiles(finish)
    for u in range(2 * steps - 3, 2 * steps):
        for d in range(2):
            rs_copy(d, u // steps, u % steps, arrived_sum(u // steps, u % steps)).wait_send()


def solution(mesh):
    n = mesh.shape["tp"]

    def step(x, w_gate, w_up, w_down):
        (m, d_model), ff = x.shape, w_gate.shape[1]
        rc = m // 2
        steps = n - 1
        hbm = pl.BlockSpec(memory_space=pltpu.HBM)
        return pl.pallas_call(
            functools.partial(kernel, n),
            out_shape=jax.ShapeDtypeStruct(x.shape, BF16),
            in_specs=[hbm] * 4,
            out_specs=pl.BlockSpec(memory_space=pltpu.VMEM),
            scratch_shapes=[
                pltpu.VMEM((2 * n * rc, d_model), BF16),
                pltpu.VMEM((2 * n * rc, ff), BF16),
                pltpu.VMEM((ff, d_model), BF16),
                pltpu.VMEM((SLOTS, d_model // 2, 2 * FT), BF16),
                pltpu.VMEM((rc, d_model), F32),
                pltpu.SemaphoreType.DMA((2, 2 * steps)),
                pltpu.SemaphoreType.DMA((2, 2 * steps)),
                pltpu.SemaphoreType.DMA((2, 2 * steps)),
                pltpu.SemaphoreType.DMA((2, 2 * steps)),
                pltpu.SemaphoreType.DMA((2, SLOTS)),
                pltpu.SemaphoreType.DMA,
                pltpu.SemaphoreType.DMA((2,)),
            ],
            compiler_params=pltpu.CompilerParams(
                collective_id=0, has_side_effects=True, vmem_limit_bytes=VMEM_LIMIT
            ),
            name="mlp_ring",
        )(x, w_gate, w_up, w_down)

    return jax.shard_map(
        step,
        mesh=mesh,
        in_specs=(P(("dp", "tp"), None), P(None, "tp"), P(None, "tp"), P("tp", None)),
        out_specs=P(("dp", "tp"), None),
        check_vma=False,
    )
```

```python
import functools

import jax
import jax.numpy as jnp
from jax import lax
from jax.experimental import pallas as pl
from jax.experimental.pallas import tpu as pltpu
from jax.sharding import PartitionSpec as P

MESH = pl.DeviceIdType.MESH
F32 = jnp.float32
BF16 = jnp.bfloat16
FT = 128
SLOTS = 4
TILT = 8
NT = 1024
VMEM_LIMIT = 51 * 1024 * 1024


def kernel(
    n, x_ref, wg_ref, wu_ref, wd_ref, y_ref,
    buf, hid, wd, wt, own, ag_send, ag_recv, rs_send, rs_recv, tilt_sem, w_sem, wd_sem, x_sem,
):
    me = lax.axis_index("tp")
    right, left = lax.rem(me + 1, n), lax.rem(me + n - 1, n)
    steps = n - 1
    rc = x_ref.shape[0] // 2
    pc = rc // 2
    d_model = x_ref.shape[1]
    ff = wg_ref.shape[1]
    tiles = ff // FT
    per = tiles // 2
    n_tiles = 2 * n * per

    def rows(block, part=0, size=pc):
        return pl.ds(pl.multiple_of(block * rc + part * pc, pc), size)

    def own_block(c):
        return 2 * n - 1 - n * c

    def ag_copy(d, c, i, src):
        return pltpu.make_async_remote_copy(
            src_ref=buf.at[src],
            dst_ref=buf.at[rows(c * n + i, d)],
            send_sem=ag_send.at[d, c * steps + i],
            recv_sem=ag_recv.at[d, c * steps + i],
            device_id={"tp": (right, left)[d]},
            device_id_type=MESH,
        )

    far = (1, steps - 1)
    before_far = 2 * steps - 3

    def short_copy():
        block = far[0] * n + far[1]
        return pltpu.make_async_remote_copy(
            src_ref=buf.at[pl.ds((block - 2) * rc, pc - TILT)],
            dst_ref=buf.at[pl.ds(block * rc, pc - TILT)],
            send_sem=ag_send.at[0, 2 * steps - 1],
            recv_sem=ag_recv.at[0, 2 * steps - 1],
            device_id={"tp": right},
            device_id_type=MESH,
        )

    def tilt_copy():
        block = far[0] * n + far[1]
        return pltpu.make_async_remote_copy(
            src_ref=buf.at[pl.ds(block * rc - TILT, TILT)],
            dst_ref=buf.at[pl.ds(block * rc + pc - TILT, TILT)],
            send_sem=tilt_sem.at[0],
            recv_sem=tilt_sem.at[1],
            device_id={"tp": left},
            device_id_type=MESH,
        )

    def arrived_sum(c, r):
        return c * n + r

    def rs_copy(d, c, r, block):
        return pltpu.make_async_remote_copy(
            src_ref=buf.at[rows(block, d)],
            dst_ref=buf.at[rows(arrived_sum(c, r), d)],
            send_sem=rs_send.at[d, c * steps + r],
            recv_sem=rs_recv.at[d, c * steps + r],
            device_id={"tp": (left, right)[d]},
            device_id_type=MESH,
        )

    def w_copies(g):
        slot = g % SLOTS
        col = pl.ds(pl.multiple_of((g % tiles) * FT, FT), FT)
        return [
            pltpu.make_async_copy(ref.at[:, col], wt.at[slot, :, pl.ds(k * FT, FT)], w_sem.at[k, slot])
            for k, ref in enumerate((wg_ref, wu_ref))
        ]

    x_copies = [
        pltpu.make_async_copy(
            x_ref.at[pl.ds(c * rc + p * pc, pc)], buf.at[rows(own_block(c), p)], x_sem.at[c, p]
        )
        for c in range(2)
        for p in range(2)
    ]
    for copy in x_copies:
        copy.start()

    barrier = pltpu.get_barrier_semaphore()
    for neighbour in (left, right):
        pl.semaphore_signal(barrier, inc=1, device_id={"tp": neighbour}, device_id_type=MESH)
    pl.semaphore_wait(barrier, 2)

    for d in range(2):
        x_copies[d].wait()
        ag_copy(d, 0, 0, rows(own_block(0), d)).start()
    for d in range(2):
        ag_copy(d, 0, 1, rows(own_block(0), 1 - d)).start()
    for copy in x_copies[2:]:
        copy.wait()
    for g in range(SLOTS - 1):
        for copy in w_copies(g):
            copy.start()
    wd_copy = pltpu.make_async_copy(wd_ref, wd, wd_sem)
    wd_copy.start()

    def hidden_half(q):
        lhs = pl.ds(pl.multiple_of((q // 2) * 2 * rc, 2 * rc), 2 * rc)

        @pl.loop(0, per)
        def _(j):
            g = q * per + j
            for copy in w_copies(g):
                copy.wait()

            @pl.when(g + SLOTS - 1 < n_tiles)
            def _():
                for copy in w_copies(g + SLOTS - 1):
                    copy.start()

            both = jnp.dot(buf[lhs, :], wt[g % SLOTS], preferred_element_type=F32)
            gate, up = both[:, :FT], both[:, FT:]
            col = pl.ds(pl.multiple_of((g % tiles) * FT, FT), FT)
            hid[lhs, col] = (jax.nn.silu(gate) * up).astype(BF16)

    def down(block, col):
        return jnp.dot(hid[rows(block, 0, rc), :], wd[:, col], preferred_element_type=F32)

    def down_tiles(body):
        @pl.loop(0, d_model // NT)
        def _(j):
            body(pl.ds(pl.multiple_of(j * NT, NT), NT))

    def multiply(block):
        def body(col):
            own[:, col] = down(block, col)

        down_tiles(body)

    def send_sum(c, r, add):
        block = arrived_sum(c, r - 2) if add else c * n + n - 2 + r
        for d in range(2):
            if add:
                rs_copy(d, c, r - 2, block).wait_recv()
            dst = rows(block, d)
            half = pl.ds(d * pc, pc)

            def body(col):
                term = own[half, col]
                if add:
                    term = term + buf[dst, col].astype(F32)
                buf[dst, col] = term.astype(BF16)

            down_tiles(body)
            rs_copy(d, c, r, block).start()

    def wait_sum(c, r):
        for d in range(2):
            rs_copy(d, c, r, arrived_sum(c, r)).wait_recv()

    def swapped(block, col):
        return jnp.concatenate([buf[rows(block, 1), col], buf[rows(block, 0), col]], axis=0).astype(F32)

    @pl.loop(0, 4 * steps - 2)
    def _(t):
        @pl.when(t < 2 * steps)
        def _():
            c, i = t // steps, t % steps
            ag_copy(1, c, i, rows(c * n + i, 1)).wait_recv()

            @pl.when(i < steps - 2)
            def _():
                ag_copy(1, c, i + 2, rows(c * n + i, 1)).start()

            @pl.when(t == before_far + 1)
            def _():
                tilt_copy().start()

            @pl.when(t < 2 * steps - 1)
            def _():
                ag_copy(0, c, i, rows(c * n + i, 0)).wait_recv()

            @pl.when(t == 2 * steps - 1)
            def _():
                short_copy().wait_recv()

            @pl.when((i < steps - 2) & (t != before_far))
            def _():
                ag_copy(0, c, i + 2, rows(c * n + i, 0)).start()

            @pl.when(t == before_far)
            def _():
                short_copy().start()

        @pl.when(t == steps - 2)
        def _():
            for i in range(2):
                for d in range(2):
                    ag_copy(d, 1, i, rows(own_block(1), i ^ d)).start()

        @pl.when((t >= 1) & (t <= 2 * steps))
        def _():
            a = t - 1
            src = (a // steps) * n + a % steps
            ag_copy(1, a // steps, a % steps, rows(src, 1)).wait_send()

            @pl.when(t < 2 * steps)
            def _():
                ag_copy(0, a // steps, a % steps, rows(src, 0)).wait_send()

        @pl.when(t == 2 * steps)
        def _():
            short_copy().wait_send()
            tilt_copy().wait()

        @pl.when(t >= 2 * steps + 1)
        def _():
            u = t - (2 * steps + 1)
            for d in range(2):
                rs_copy(d, u // steps, u % steps, arrived_sum(u // steps, u % steps)).wait_send()

        @pl.when(t >= 2 * steps - 2)
        def _():
            u = t - (2 * steps - 2)
            c, r = u // steps, u % steps

            @pl.when(r < 2)
            def _():
                send_sum(c, r, False)

            @pl.when(r >= 2)
            def _():
                send_sum(c, r, True)

        @pl.when((t >= 1) & (t <= 2 * n))
        def _():
            hidden_half(t - 1)

        @pl.when(t == 2 * steps - 3)
        def _():
            wd_copy.wait()

        @pl.when((t >= 2 * steps - 3) & (t < 4 * steps - 3))
        def _():
            u = t - (2 * steps - 3)
            multiply(u // steps * n + n - 2 - u % steps)

        @pl.when(t == 3 * steps - 1)
        def _():
            wait_sum(0, steps - 2)
            wait_sum(0, steps - 1)
            last = arrived_sum(0, steps - 1)
            dst = rows(last, 0, rc)

            def body(col):
                total = down(own_block(0), col) + swapped(last - 1, col) + buf[dst, col].astype(F32)
                y_ref[pl.ds(0, rc), col] = total.astype(BF16)

            down_tiles(body)

    multiply(own_block(1))
    wait_sum(1, steps - 2)
    last = arrived_sum(1, steps - 1)

    def partial(col):
        own[:, col] = own[:, col] + swapped(last - 1, col)

    down_tiles(partial)
    for d in range(2):
        rs_copy(d, 1, steps - 1, last).wait_recv()
        half = pl.ds(d * pc, pc)

        def finish(col):
            y_ref[pl.ds(rc + d * pc, pc), col] = (own[half, col] + buf[rows(last, d), col].astype(F32)).astype(BF16)

        down_tiles(finish)

    for u in range(2 * steps - 3, 2 * steps):
        for d in range(2):
            rs_copy(d, u // steps, u % steps, arrived_sum(u // steps, u % steps)).wait_send()


def solution(mesh):
    n = mesh.shape["tp"]

    def step(x, w_gate, w_up, w_down):
        (m, d_model), ff = x.shape, w_gate.shape[1]
        rc = m // 2
        steps = n - 1
        hbm = pl.BlockSpec(memory_space=pltpu.HBM)
        return pl.pallas_call(
            functools.partial(kernel, n),
            out_shape=jax.ShapeDtypeStruct(x.shape, BF16),
            in_specs=[hbm] * 4,
            out_specs=pl.BlockSpec(memory_space=pltpu.VMEM),
            scratch_shapes=[
                pltpu.VMEM((2 * n * rc, d_model), BF16),
                pltpu.VMEM((2 * n * rc, ff), BF16),
                pltpu.VMEM((ff, d_model), BF16),
                pltpu.VMEM((SLOTS, d_model, 2 * FT), BF16),
                pltpu.VMEM((rc, d_model), F32),
                pltpu.SemaphoreType.DMA((2, 2 * steps)),
                pltpu.SemaphoreType.DMA((2, 2 * steps)),
                pltpu.SemaphoreType.DMA((2, 2 * steps)),
                pltpu.SemaphoreType.DMA((2, 2 * steps)),
                pltpu.SemaphoreType.DMA((2,)),
                pltpu.SemaphoreType.DMA((2, SLOTS)),
                pltpu.SemaphoreType.DMA,
                pltpu.SemaphoreType.DMA((2, 2)),
            ],
            compiler_params=pltpu.CompilerParams(
                collective_id=0, has_side_effects=True, vmem_limit_bytes=VMEM_LIMIT
            ),
            name="mlp_ring",
        )(x, w_gate, w_up, w_down)

    return jax.shard_map(
        step,
        mesh=mesh,
        in_specs=(P(("dp", "tp"), None), P(None, "tp"), P(None, "tp"), P("tp", None)),
        out_specs=P(("dp", "tp"), None),
        check_vma=False,
    )
```

```python
import functools

import jax
import jax.numpy as jnp
from jax import lax
from jax.experimental import pallas as pl
from jax.experimental.pallas import tpu as pltpu
from jax.sharding import PartitionSpec as P

MESH = pl.DeviceIdType.MESH
F32 = jnp.float32
BF16 = jnp.bfloat16
FT = 128
SLOTS = 4
TILT = 8
NT = 1024
VMEM_LIMIT = 51 * 1024 * 1024


def kernel(
    n, x_ref, wg_ref, wu_ref, wd_ref, y_ref,
    buf, hid, wd, wt, own, ag_send, ag_recv, rs_send, rs_recv, tilt_sem, w_sem, wd_sem, x_sem,
):
    me = lax.axis_index("tp")
    right, left = lax.rem(me + 1, n), lax.rem(me + n - 1, n)
    steps = n - 1
    rc = x_ref.shape[0] // 2
    pc = rc // 2
    d_model = x_ref.shape[1]
    ff = wg_ref.shape[1]
    tiles = ff // FT
    per = tiles // 2
    n_tiles = 2 * n * per

    def rows(block, part=0, size=pc):
        return pl.ds(pl.multiple_of(block * rc + part * pc, pc), size)

    def own_block(c):
        return 2 * n - 1 - n * c

    def ag_copy(d, c, i, src):
        return pltpu.make_async_remote_copy(
            src_ref=buf.at[src],
            dst_ref=buf.at[rows(c * n + i, d)],
            send_sem=ag_send.at[d, c * steps + i],
            recv_sem=ag_recv.at[d, c * steps + i],
            device_id={"tp": (right, left)[d]},
            device_id_type=MESH,
        )

    far = (1, steps - 1)
    before_far = 2 * steps - 3

    def short_copy():
        block = far[0] * n + far[1]
        return pltpu.make_async_remote_copy(
            src_ref=buf.at[pl.ds((block - 2) * rc, pc - TILT)],
            dst_ref=buf.at[pl.ds(block * rc, pc - TILT)],
            send_sem=ag_send.at[0, 2 * steps - 1],
            recv_sem=ag_recv.at[0, 2 * steps - 1],
            device_id={"tp": right},
            device_id_type=MESH,
        )

    split = d_model * 3 // 4

    def tilt_copy(d):
        block = far[0] * n + far[1]
        src = ((block - 2) * rc + pc, block * rc)[d] - TILT
        col = (pl.ds(split, d_model - split), pl.ds(0, split))[d]
        return pltpu.make_async_remote_copy(
            src_ref=buf.at[pl.ds(src, TILT), col],
            dst_ref=buf.at[pl.ds(block * rc + pc - TILT, TILT), col],
            send_sem=tilt_sem.at[0, d],
            recv_sem=tilt_sem.at[1, d],
            device_id={"tp": (right, left)[d]},
            device_id_type=MESH,
        )

    def arrived_sum(c, r):
        return c * n + r

    def rs_copy(d, c, r, block):
        return pltpu.make_async_remote_copy(
            src_ref=buf.at[rows(block, d)],
            dst_ref=buf.at[rows(arrived_sum(c, r), d)],
            send_sem=rs_send.at[d, c * steps + r],
            recv_sem=rs_recv.at[d, c * steps + r],
            device_id={"tp": (left, right)[d]},
            device_id_type=MESH,
        )

    def w_copies(g):
        slot = g % SLOTS
        col = pl.ds(pl.multiple_of((g % tiles) * FT, FT), FT)
        return [
            pltpu.make_async_copy(ref.at[:, col], wt.at[slot, :, pl.ds(k * FT, FT)], w_sem.at[k, slot])
            for k, ref in enumerate((wg_ref, wu_ref))
        ]

    x_copies = [
        pltpu.make_async_copy(
            x_ref.at[pl.ds(c * rc + p * pc, pc)], buf.at[rows(own_block(c), p)], x_sem.at[c, p]
        )
        for c in range(2)
        for p in range(2)
    ]
    for copy in x_copies:
        copy.start()

    barrier = pltpu.get_barrier_semaphore()
    for neighbour in (left, right):
        pl.semaphore_signal(barrier, inc=1, device_id={"tp": neighbour}, device_id_type=MESH)
    pl.semaphore_wait(barrier, 2)

    for d in range(2):
        x_copies[d].wait()
        ag_copy(d, 0, 0, rows(own_block(0), d)).start()
    for d in range(2):
        ag_copy(d, 0, 1, rows(own_block(0), 1 - d)).start()
    for copy in x_copies[2:]:
        copy.wait()
    for g in range(SLOTS - 1):
        for copy in w_copies(g):
            copy.start()
    wd_copy = pltpu.make_async_copy(wd_ref, wd, wd_sem)
    wd_copy.start()

    def hidden_half(q):
        lhs = pl.ds(pl.multiple_of((q // 2) * 2 * rc, 2 * rc), 2 * rc)

        @pl.loop(0, per)
        def _(j):
            g = q * per + j
            for copy in w_copies(g):
                copy.wait()

            @pl.when(g + SLOTS - 1 < n_tiles)
            def _():
                for copy in w_copies(g + SLOTS - 1):
                    copy.start()

            both = jnp.dot(buf[lhs, :], wt[g % SLOTS], preferred_element_type=F32)
            gate, up = both[:, :FT], both[:, FT:]
            col = pl.ds(pl.multiple_of((g % tiles) * FT, FT), FT)
            hid[lhs, col] = (jax.nn.silu(gate) * up).astype(BF16)

    def down(block, col):
        return jnp.dot(hid[rows(block, 0, rc), :], wd[:, col], preferred_element_type=F32)

    def down_tiles(body):
        @pl.loop(0, d_model // NT)
        def _(j):
            body(pl.ds(pl.multiple_of(j * NT, NT), NT))

    def multiply(block):
        def body(col):
            own[:, col] = down(block, col)

        down_tiles(body)

    def send_sum(c, r, add):
        block = arrived_sum(c, r - 2) if add else c * n + n - 2 + r
        for d in range(2):
            if add:
                rs_copy(d, c, r - 2, block).wait_recv()
            dst = rows(block, d)
            half = pl.ds(d * pc, pc)

            def body(col):
                term = own[half, col]
                if add:
                    term = term + buf[dst, col].astype(F32)
                buf[dst, col] = term.astype(BF16)

            down_tiles(body)
            rs_copy(d, c, r, block).start()

    def wait_sum(c, r):
        for d in range(2):
            rs_copy(d, c, r, arrived_sum(c, r)).wait_recv()

    def swapped(block, col):
        return jnp.concatenate([buf[rows(block, 1), col], buf[rows(block, 0), col]], axis=0).astype(F32)

    @pl.loop(0, 4 * steps - 2)
    def _(t):
        @pl.when(t < 2 * steps)
        def _():
            c, i = t // steps, t % steps
            ag_copy(1, c, i, rows(c * n + i, 1)).wait_recv()

            @pl.when(i < steps - 2)
            def _():
                ag_copy(1, c, i + 2, rows(c * n + i, 1)).start()

            @pl.when(t == before_far + 1)
            def _():
                tilt_copy(1).start()

            @pl.when(t < 2 * steps - 1)
            def _():
                ag_copy(0, c, i, rows(c * n + i, 0)).wait_recv()

            @pl.when(t == 2 * steps - 1)
            def _():
                short_copy().wait_recv()

            @pl.when((i < steps - 2) & (t != before_far))
            def _():
                ag_copy(0, c, i + 2, rows(c * n + i, 0)).start()

            @pl.when(t == before_far)
            def _():
                short_copy().start()
                tilt_copy(0).start()

        @pl.when(t == steps - 2)
        def _():
            for i in range(2):
                for d in range(2):
                    ag_copy(d, 1, i, rows(own_block(1), i ^ d)).start()

        @pl.when((t >= 1) & (t <= 2 * steps))
        def _():
            a = t - 1
            src = (a // steps) * n + a % steps
            ag_copy(1, a // steps, a % steps, rows(src, 1)).wait_send()

            @pl.when(t < 2 * steps)
            def _():
                ag_copy(0, a // steps, a % steps, rows(src, 0)).wait_send()

        @pl.when(t == 2 * steps)
        def _():
            short_copy().wait_send()
            for d in range(2):
                tilt_copy(d).wait()

        @pl.when(t >= 2 * steps + 1)
        def _():
            u = t - (2 * steps + 1)
            for d in range(2):
                rs_copy(d, u // steps, u % steps, arrived_sum(u // steps, u % steps)).wait_send()

        @pl.when(t >= 2 * steps - 2)
        def _():
            u = t - (2 * steps - 2)
            c, r = u // steps, u % steps

            @pl.when(r < 2)
            def _():
                send_sum(c, r, False)

            @pl.when(r >= 2)
            def _():
                send_sum(c, r, True)

        @pl.when((t >= 1) & (t <= 2 * n))
        def _():
            hidden_half(t - 1)

        @pl.when(t == 2 * steps - 3)
        def _():
            wd_copy.wait()

        @pl.when((t >= 2 * steps - 3) & (t < 4 * steps - 3))
        def _():
            u = t - (2 * steps - 3)
            multiply(u // steps * n + n - 2 - u % steps)

        @pl.when(t == 3 * steps - 1)
        def _():
            wait_sum(0, steps - 2)
            wait_sum(0, steps - 1)
            last = arrived_sum(0, steps - 1)
            dst = rows(last, 0, rc)

            def body(col):
                total = down(own_block(0), col) + swapped(last - 1, col) + buf[dst, col].astype(F32)
                y_ref[pl.ds(0, rc), col] = total.astype(BF16)

            down_tiles(body)

    multiply(own_block(1))
    wait_sum(1, steps - 2)
    last = arrived_sum(1, steps - 1)

    def partial(col):
        own[:, col] = own[:, col] + swapped(last - 1, col)

    down_tiles(partial)
    for d in range(2):
        rs_copy(d, 1, steps - 1, last).wait_recv()
        half = pl.ds(d * pc, pc)

        def finish(col):
            y_ref[pl.ds(rc + d * pc, pc), col] = (own[half, col] + buf[rows(last, d), col].astype(F32)).astype(BF16)

        down_tiles(finish)

    for u in range(2 * steps - 3, 2 * steps):
        for d in range(2):
            rs_copy(d, u // steps, u % steps, arrived_sum(u // steps, u % steps)).wait_send()


def solution(mesh):
    n = mesh.shape["tp"]

    def step(x, w_gate, w_up, w_down):
        (m, d_model), ff = x.shape, w_gate.shape[1]
        rc = m // 2
        steps = n - 1
        hbm = pl.BlockSpec(memory_space=pltpu.HBM)
        return pl.pallas_call(
            functools.partial(kernel, n),
            out_shape=jax.ShapeDtypeStruct(x.shape, BF16),
            in_specs=[hbm] * 4,
            out_specs=pl.BlockSpec(memory_space=pltpu.VMEM),
            scratch_shapes=[
                pltpu.VMEM((2 * n * rc, d_model), BF16),
                pltpu.VMEM((2 * n * rc, ff), BF16),
                pltpu.VMEM((ff, d_model), BF16),
                pltpu.VMEM((SLOTS, d_model, 2 * FT), BF16),
                pltpu.VMEM((rc, d_model), F32),
                pltpu.SemaphoreType.DMA((2, 2 * steps)),
                pltpu.SemaphoreType.DMA((2, 2 * steps)),
                pltpu.SemaphoreType.DMA((2, 2 * steps)),
                pltpu.SemaphoreType.DMA((2, 2 * steps)),
                pltpu.SemaphoreType.DMA((2, 2)),
                pltpu.SemaphoreType.DMA((2, SLOTS)),
                pltpu.SemaphoreType.DMA,
                pltpu.SemaphoreType.DMA((2, 2)),
            ],
            compiler_params=pltpu.CompilerParams(
                collective_id=0, has_side_effects=True, vmem_limit_bytes=VMEM_LIMIT
            ),
            name="mlp_ring",
        )(x, w_gate, w_up, w_down)

    return jax.shard_map(
        step,
        mesh=mesh,
        in_specs=(P(("dp", "tp"), None), P(None, "tp"), P(None, "tp"), P("tp", None)),
        out_specs=P(("dp", "tp"), None),
        check_vma=False,
    )
```

```python
import functools

import jax
import jax.numpy as jnp
from jax import lax
from jax.experimental import pallas as pl
from jax.experimental.pallas import tpu as pltpu
from jax.sharding import PartitionSpec as P

MESH = pl.DeviceIdType.MESH
F32 = jnp.float32
BF16 = jnp.bfloat16
FT = 128
SLOTS = 4
TILT = 8
NT = 1024
VMEM_LIMIT = 51 * 1024 * 1024


def kernel(
    n, x_ref, wg_ref, wu_ref, wd_ref, y_ref,
    buf, hid, wd, wt, own, ag_send, ag_recv, rs_send, rs_recv, tilt_sem, w_sem, wd_sem, x_sem,
):
    me = lax.axis_index("tp")
    right, left = lax.rem(me + 1, n), lax.rem(me + n - 1, n)
    steps = n - 1
    rc = x_ref.shape[0] // 2
    pc = rc // 2
    d_model = x_ref.shape[1]
    ff = wg_ref.shape[1]
    tiles = ff // FT
    per = tiles // 2
    n_tiles = 2 * n * per

    def rows(block, part=0, size=pc):
        return pl.ds(pl.multiple_of(block * rc + part * pc, pc), size)

    def own_block(c):
        return 2 * n - 1 - n * c

    def ag_copy(d, c, i, src):
        return pltpu.make_async_remote_copy(
            src_ref=buf.at[src],
            dst_ref=buf.at[rows(c * n + i, d)],
            send_sem=ag_send.at[d, c * steps + i],
            recv_sem=ag_recv.at[d, c * steps + i],
            device_id={"tp": (right, left)[d]},
            device_id_type=MESH,
        )

    far = (1, steps - 1)
    before_far = 2 * steps - 3

    def short_copy():
        block = far[0] * n + far[1]
        return pltpu.make_async_remote_copy(
            src_ref=buf.at[pl.ds((block - 2) * rc, pc - TILT)],
            dst_ref=buf.at[pl.ds(block * rc, pc - TILT)],
            send_sem=ag_send.at[0, 2 * steps - 1],
            recv_sem=ag_recv.at[0, 2 * steps - 1],
            device_id={"tp": right},
            device_id_type=MESH,
        )

    split = d_model * 3 // 4

    def tilt_copy(d):
        block = far[0] * n + far[1]
        src = ((block - 2) * rc + pc, block * rc)[d] - TILT
        col = (pl.ds(split, d_model - split), pl.ds(0, split))[d]
        return pltpu.make_async_remote_copy(
            src_ref=buf.at[pl.ds(src, TILT), col],
            dst_ref=buf.at[pl.ds(block * rc + pc - TILT, TILT), col],
            send_sem=tilt_sem.at[0, d],
            recv_sem=tilt_sem.at[1, d],
            device_id={"tp": (right, left)[d]},
            device_id_type=MESH,
        )

    def arrived_sum(c, r):
        return c * n + r

    def rs_copy(d, c, r, block):
        return pltpu.make_async_remote_copy(
            src_ref=buf.at[rows(block, d)],
            dst_ref=buf.at[rows(arrived_sum(c, r), d)],
            send_sem=rs_send.at[d, c * steps + r],
            recv_sem=rs_recv.at[d, c * steps + r],
            device_id={"tp": (left, right)[d]},
            device_id_type=MESH,
        )

    def w_copies(g):
        slot = g % SLOTS
        col = pl.ds(pl.multiple_of((g % tiles) * FT, FT), FT)
        return [
            pltpu.make_async_copy(ref.at[:, col], wt.at[slot, :, pl.ds(k * FT, FT)], w_sem.at[k, slot])
            for k, ref in enumerate((wg_ref, wu_ref))
        ]

    x_copies = [
        pltpu.make_async_copy(
            x_ref.at[pl.ds(c * rc + p * pc, pc)], buf.at[rows(own_block(c), p)], x_sem.at[c, p]
        )
        for c in range(2)
        for p in range(2)
    ]
    for copy in x_copies:
        copy.start()

    barrier = pltpu.get_barrier_semaphore()
    for neighbour in (left, right):
        pl.semaphore_signal(barrier, inc=1, device_id={"tp": neighbour}, device_id_type=MESH)
    pl.semaphore_wait(barrier, 2)

    for d in range(2):
        x_copies[d].wait()
        ag_copy(d, 0, 0, rows(own_block(0), d)).start()
    for d in range(2):
        ag_copy(d, 0, 1, rows(own_block(0), 1 - d)).start()
    for copy in x_copies[2:]:
        copy.wait()
    for g in range(SLOTS - 1):
        for copy in w_copies(g):
            copy.start()
    wd_copy = pltpu.make_async_copy(wd_ref, wd, wd_sem)
    wd_copy.start(priority=1)

    def hidden_half(q):
        lhs = pl.ds(pl.multiple_of((q // 2) * 2 * rc, 2 * rc), 2 * rc)

        @pl.loop(0, per)
        def _(j):
            g = q * per + j
            for copy in w_copies(g):
                copy.wait()

            @pl.when(g + SLOTS - 1 < n_tiles)
            def _():
                for copy in w_copies(g + SLOTS - 1):
                    copy.start(priority=1)

            both = jnp.dot(buf[lhs, :], wt[g % SLOTS], preferred_element_type=F32)
            gate, up = both[:, :FT], both[:, FT:]
            col = pl.ds(pl.multiple_of((g % tiles) * FT, FT), FT)
            hid[lhs, col] = (jax.nn.silu(gate) * up).astype(BF16)

    def down(block, col):
        return jnp.dot(hid[rows(block, 0, rc), :], wd[:, col], preferred_element_type=F32)

    def down_tiles(body):
        @pl.loop(0, d_model // NT)
        def _(j):
            body(pl.ds(pl.multiple_of(j * NT, NT), NT))

    def multiply(block):
        def body(col):
            own[:, col] = down(block, col)

        down_tiles(body)

    def send_sum(c, r, add):
        block = arrived_sum(c, r - 2) if add else c * n + n - 2 + r
        for d in range(2):
            if add:
                rs_copy(d, c, r - 2, block).wait_recv()
            dst = rows(block, d)
            half = pl.ds(d * pc, pc)

            def body(col):
                term = own[half, col]
                if add:
                    term = term + buf[dst, col].astype(F32)
                buf[dst, col] = term.astype(BF16)

            down_tiles(body)
            rs_copy(d, c, r, block).start()

    def wait_sum(c, r):
        for d in range(2):
            rs_copy(d, c, r, arrived_sum(c, r)).wait_recv()

    def swapped(block, col):
        return jnp.concatenate([buf[rows(block, 1), col], buf[rows(block, 0), col]], axis=0).astype(F32)

    @pl.loop(0, 4 * steps - 2)
    def _(t):
        @pl.when(t < 2 * steps)
        def _():
            c, i = t // steps, t % steps
            ag_copy(1, c, i, rows(c * n + i, 1)).wait_recv()

            @pl.when(i < steps - 2)
            def _():
                ag_copy(1, c, i + 2, rows(c * n + i, 1)).start()

            @pl.when(t == before_far + 1)
            def _():
                tilt_copy(1).start()

            @pl.when(t < 2 * steps - 1)
            def _():
                ag_copy(0, c, i, rows(c * n + i, 0)).wait_recv()

            @pl.when(t == 2 * steps - 1)
            def _():
                short_copy().wait_recv()

            @pl.when((i < steps - 2) & (t != before_far))
            def _():
                ag_copy(0, c, i + 2, rows(c * n + i, 0)).start()

            @pl.when(t == before_far)
            def _():
                short_copy().start()
                tilt_copy(0).start()

        @pl.when(t == steps - 2)
        def _():
            for i in range(2):
                for d in range(2):
                    ag_copy(d, 1, i, rows(own_block(1), i ^ d)).start()

        @pl.when((t >= 1) & (t <= 2 * steps))
        def _():
            a = t - 1
            src = (a // steps) * n + a % steps
            ag_copy(1, a // steps, a % steps, rows(src, 1)).wait_send()

            @pl.when(t < 2 * steps)
            def _():
                ag_copy(0, a // steps, a % steps, rows(src, 0)).wait_send()

        @pl.when(t == 2 * steps)
        def _():
            short_copy().wait_send()
            for d in range(2):
                tilt_copy(d).wait()

        @pl.when(t >= 2 * steps + 1)
        def _():
            u = t - (2 * steps + 1)
            for d in range(2):
                rs_copy(d, u // steps, u % steps, arrived_sum(u // steps, u % steps)).wait_send()

        @pl.when(t >= 2 * steps - 2)
        def _():
            u = t - (2 * steps - 2)
            c, r = u // steps, u % steps

            @pl.when(r < 2)
            def _():
                send_sum(c, r, False)

            @pl.when(r >= 2)
            def _():
                send_sum(c, r, True)

        @pl.when((t >= 1) & (t <= 2 * n))
        def _():
            hidden_half(t - 1)

        @pl.when(t == 2 * steps - 3)
        def _():
            wd_copy.wait()

        @pl.when((t >= 2 * steps - 3) & (t < 4 * steps - 3))
        def _():
            u = t - (2 * steps - 3)
            multiply(u // steps * n + n - 2 - u % steps)

        @pl.when(t == 3 * steps - 1)
        def _():
            wait_sum(0, steps - 2)
            wait_sum(0, steps - 1)
            last = arrived_sum(0, steps - 1)
            dst = rows(last, 0, rc)

            def body(col):
                total = down(own_block(0), col) + swapped(last - 1, col) + buf[dst, col].astype(F32)
                y_ref[pl.ds(0, rc), col] = total.astype(BF16)

            down_tiles(body)

    multiply(own_block(1))
    wait_sum(1, steps - 2)
    last = arrived_sum(1, steps - 1)

    def partial(col):
        own[:, col] = own[:, col] + swapped(last - 1, col)

    down_tiles(partial)
    for d in range(2):
        rs_copy(d, 1, steps - 1, last).wait_recv()
        half = pl.ds(d * pc, pc)

        def finish(col):
            y_ref[pl.ds(rc + d * pc, pc), col] = (own[half, col] + buf[rows(last, d), col].astype(F32)).astype(BF16)

        down_tiles(finish)

    for u in range(2 * steps - 3, 2 * steps):
        for d in range(2):
            rs_copy(d, u // steps, u % steps, arrived_sum(u // steps, u % steps)).wait_send()


def solution(mesh):
    n = mesh.shape["tp"]

    def step(x, w_gate, w_up, w_down):
        (m, d_model), ff = x.shape, w_gate.shape[1]
        rc = m // 2
        steps = n - 1
        hbm = pl.BlockSpec(memory_space=pltpu.HBM)
        return pl.pallas_call(
            functools.partial(kernel, n),
            out_shape=jax.ShapeDtypeStruct(x.shape, BF16),
            in_specs=[hbm] * 4,
            out_specs=pl.BlockSpec(memory_space=pltpu.VMEM),
            scratch_shapes=[
                pltpu.VMEM((2 * n * rc, d_model), BF16),
                pltpu.VMEM((2 * n * rc, ff), BF16),
                pltpu.VMEM((ff, d_model), BF16),
                pltpu.VMEM((SLOTS, d_model, 2 * FT), BF16),
                pltpu.VMEM((rc, d_model), F32),
                pltpu.SemaphoreType.DMA((2, 2 * steps)),
                pltpu.SemaphoreType.DMA((2, 2 * steps)),
                pltpu.SemaphoreType.DMA((2, 2 * steps)),
                pltpu.SemaphoreType.DMA((2, 2 * steps)),
                pltpu.SemaphoreType.DMA((2, 2)),
                pltpu.SemaphoreType.DMA((2, SLOTS)),
                pltpu.SemaphoreType.DMA,
                pltpu.SemaphoreType.DMA((2, 2)),
            ],
            compiler_params=pltpu.CompilerParams(
                collective_id=0, has_side_effects=True, vmem_limit_bytes=VMEM_LIMIT
            ),
            name="mlp_ring",
        )(x, w_gate, w_up, w_down)

    return jax.shard_map(
        step,
        mesh=mesh,
        in_specs=(P(("dp", "tp"), None), P(None, "tp"), P(None, "tp"), P("tp", None)),
        out_specs=P(("dp", "tp"), None),
        check_vma=False,
    )
```
